8 devices in a mesh: row: 2 (over z, y), col: 4 (over x, core).
Axes of the slice: x: 2, y: 2, z: 1, core: 2. Of those that a mesh axis runs over, the one named last changes fastest.
Arguments:
- v_panels: float32 [6144, 6144], P('row', 'col')
- t_factors: float32 [96, 64, 64], P('col')
- z_vectors: float32 [6144, 2048], P(None, ('col', 'row'))
Outputs:
- output: float32 [6144, 2048], P('row', 'col')
All inputs are finite; a program needn't handle non-finite values.
Results may differ from the reference program's by a relative error of at most 0.001.
Values sent between devices are 32-bit elements.
A program may use at most 1 GiB of HBM per device.

```python
import jax
import jax.numpy as jnp
from jax import lax

N = 6144
B = 64
K = 2048


def build_factors(v_panels):
    panel_count = N // B
    v_blocks = v_panels.reshape(N, panel_count, B).astype(jnp.float32)
    gram_mat = jnp.einsum("nmp,nmq->mpq", v_blocks, v_blocks)
    tau_all = 2.0 / jnp.diagonal(gram_mat, axis1=1, axis2=2)
    lane_ids = jnp.arange(B)

    def add_column(col_idx, t_acc):
        g_col = lax.dynamic_index_in_dim(gram_mat, col_idx, axis=2, keepdims=False)
        g_col = jnp.where(lane_ids[None, :] < col_idx, g_col, 0.0)
        tau_col = lax.dynamic_index_in_dim(tau_all, col_idx, axis=1, keepdims=True)
        new_col = -tau_col * jnp.einsum("mpq,mq->mp", t_acc, g_col)
        new_col = jnp.where(lane_ids[None, :] == col_idx, tau_col, new_col)
        return jnp.where(lane_ids[None, None, :] == col_idx, new_col[:, :, None], t_acc)

    t_start = jnp.zeros((panel_count, B, B), jnp.float32)
    return lax.fori_loop(0, B, add_column, t_start)


def setup_inputs(seed: int = 0) -> dict:
    key = jax.random.key(seed)
    key_v, key_z = jax.random.split(key)
    raw_v = jax.random.normal(key_v, (N, N), jnp.float32)
    row_ids = jnp.arange(N)[:, None]
    col_ids = jnp.arange(N)[None, :]
    in_block = (row_ids // B) == (col_ids // B)
    scaled = raw_v * jnp.where(in_block, B ** -0.5, 1.0)
    v_panels = jnp.where(row_ids > col_ids, scaled, jnp.where(row_ids == col_ids, 1.0, 0.0)).astype(jnp.float32)
    t_factors = build_factors(v_panels)
    z_vectors = jax.random.normal(key_z, (N, K), jnp.float32)
    return {"v_panels": v_panels, "t_factors": t_factors, "z_vectors": z_vectors}


def reference(v_panels, t_factors, z_vectors):
    panel_count = N // B

    def apply_panel(step, x_cur):
        panel_idx = panel_count - 1 - step
        v_pan = lax.dynamic_slice_in_dim(v_panels, panel_idx * B, B, axis=1)
        t_pan = lax.dynamic_index_in_dim(t_factors, panel_idx, axis=0, keepdims=False)
        w_mat = lax.dot_general(v_pan, x_cur, (((0,), (0,)), ((), ())), precision=lax.Precision.HIGHEST, preferred_element_type=jnp.float32)
        y_mat = jnp.dot(t_pan, w_mat, precision=lax.Precision.HIGHEST, preferred_element_type=jnp.float32)
        return x_cur - jnp.dot(v_pan, y_mat, precision=lax.Precision.HIGHEST, preferred_element_type=jnp.float32)

    return lax.fori_loop(0, panel_count, apply_panel, z_vectors)
```

```python
import jax
import jax.numpy as jnp
from jax import lax
from jax.experimental import pallas as pl
from jax.experimental.pallas import tpu as pltpu
from jax.sharding import PartitionSpec as P

FULL = lax.Precision.HIGHEST
MESH = pl.DeviceIdType.MESH
NB = 256
TR = 512


def mm(a, b):
    return lax.dot_general(a, b, (((1,), (0,)), ((), ())), precision=FULL, preferred_element_type=jnp.float32)


def mtm(a, b):
    return lax.dot_general(a, b, (((0,), (0,)), ((), ())), precision=FULL, preferred_element_type=jnp.float32)


def kernel(
    v_ref, t_ref, z_ref, out_ref, vall,
    x, vs, tb, gown, grecv, ts, ws, wr, ys,
    far_s, far_r, sib_s, sib_r, dia_s, dia_r, t_s, t_r, w_s, w_r, z_s, z_r, g_s, g_r, loc, ld,
):
    r = lax.axis_index("row")
    c = lax.axis_index("col")
    rows = v_ref.shape[0]
    slots = v_ref.shape[1] // NB
    tiles = rows // TR
    per_row = rows // NB
    sib = c + 1 - 2 * (c % 2)
    far = (c + 2) % 4
    other = 1 - r

    barrier = pltpu.get_barrier_semaphore()
    for dst in ((r, sib), (r, far), (other, c)):
        pl.semaphore_signal(barrier, inc=1, device_id=dst, device_id_type=MESH)
    pl.semaphore_wait(barrier, 3)

    def first_tile(j):
        return lax.min(lax.max(j - per_row * r, 0) * NB // TR, tiles)

    def tile(k):
        return pl.ds(pl.multiple_of(k * TR, TR), TR)

    def each_tile(j, fn):
        def body(k, carry):
            fn(k)
            return carry

        lax.fori_loop(first_tile(j), tiles, body, 0)

    def own_tile(s, k):
        return v_ref.at[tile(k), pl.ds(pl.multiple_of(s * NB, NB), NB)]

    def remote(src, dst, ssem, rsem, to):
        return pltpu.make_async_remote_copy(src_ref=src, dst_ref=dst, send_sem=ssem, recv_sem=rsem, device_id=to, device_id_type=MESH)

    def own_copy(s, k, ssem, rsem, to):
        return remote(own_tile(s, k), vall.at[c * slots + s, tile(k)], ssem.at[s, k], rsem.at[s, k], (r, to))

    def got_copy(j, s, k, ssem, rsem, to):
        return remote(vall.at[j, tile(k)], vall.at[j, tile(k)], ssem.at[s, k], rsem.at[s, k], (r, to))

    def send_far(s):
        each_tile(c * slots + s, lambda k: own_copy(s, k, far_s, far_r, far).start())

    def loop_down(hi, n, fn):
        def body(i, carry):
            fn(hi - i)
            return carry

        lax.fori_loop(0, n, body, 0)

    zc = remote(z_ref.at[pl.ds(pl.multiple_of(other * rows, rows), rows)], x.at[r], z_s, z_r, (other, c))
    zc.start()
    zl = pltpu.make_async_copy(z_ref.at[pl.ds(pl.multiple_of(r * rows, rows), rows)], x.at[r], loc.at[0])
    zl.start()
    tl = pltpu.make_async_copy(t_ref, ts, loc.at[1])
    tl.start()

    odd = c % 2
    even = 1 - odd

    @pl.when(odd == 1)
    def _():
        loop_down(slots - 1, 3, send_far)

    loop_down(slots - 1, slots, lambda s: each_tile(c * slots + s, lambda k: own_copy(s, k, sib_s, sib_r, sib).start()))

    def gram(s):
        j = c * slots + s
        each_tile(j, lambda k: pltpu.make_async_copy(own_tile(s, k), vs.at[0, tile(k)], ld.at[k]).start())
        gown[s] = jnp.zeros((NB, NB), jnp.float32)

        def add(k):
            pltpu.make_async_copy(own_tile(s, k), vs.at[0, tile(k)], ld.at[k]).wait()
            v_t = vs[0, tile(k), :]
            gown[s] = gown[s] + mtm(v_t, v_t)

        each_tile(j, add)

    loop_down(slots - 1, slots, gram)
    tl.wait()

    def merge(s):
        j = c * slots + s
        g = gown[s]
        tb[j] = jnp.zeros((NB, NB), jnp.float32)
        for i in range(2):
            t_a, t_b = ts[4 * s + 2 * i], ts[4 * s + 2 * i + 1]
            o = 128 * i
            tb[j, o : o + 64, o : o + 64] = t_a
            tb[j, o + 64 : o + 128, o + 64 : o + 128] = t_b
            tb[j, o : o + 64, o + 64 : o + 128] = -mm(mm(t_a, g[o : o + 64, o + 64 : o + 128]), t_b)
        tb[j, 0:128, 128:256] = -mm(mm(tb[j, 0:128, 0:128], g[0:128, 128:256]), tb[j, 128:256, 128:256])

    def t_copy(q, i, to):
        part = tb.at[pl.ds(q * slots, slots)]
        return remote(part, part, t_s.at[i], t_r.at[i], (r, to))

    def factors():
        loop_down(slots - 1, slots, merge)
        t_copy(c, 0, sib).start()
        t_copy(c, 1, far).start()

    gc = remote(gown, grecv, g_s, g_r, (other, c))

    @pl.when(c < 2)
    def _():
        gc.start()

    @pl.when((c >= 2) & (r == 1))
    def _():
        factors()

    def rest_far():
        @pl.when(odd == 1)
        def _():
            loop_down(slots - 4, slots - 3, send_far)

        @pl.when(odd == 0)
        def _():
            loop_down(slots - 1, slots, send_far)

    @pl.when(c >= 2)
    def _():
        rest_far()

    def t_get(q):
        @pl.when(q == sib)
        def _():
            t_copy(q, 0, sib).wait_recv()

        @pl.when(q == far)
        def _():
            t_copy(q, 1, far).wait_recv()
            t_copy(q, 2, sib).start()

        @pl.when((q + 2) % 4 == sib)
        def _():
            t_copy(q, 2, sib).wait_recv()

    def acquire(j):
        q, s = j // slots, j % slots
        b = j % 2

        @pl.when(q == sib)
        def _():
            each_tile(j, lambda k: got_copy(j, s, k, sib_s, sib_r, sib).wait_recv())

        @pl.when(q == far)
        def _():
            def pass_on(k):
                got_copy(j, s, k, far_s, far_r, far).wait_recv()
                got_copy(j, s, k, dia_s, dia_r, sib).start()

            each_tile(j, pass_on)

        @pl.when((q + 2) % 4 == sib)
        def _():
            each_tile(j, lambda k: got_copy(j, s, k, dia_s, dia_r, sib).wait_recv())

        @pl.when(q == c)
        def _():
            each_tile(j, lambda k: pltpu.make_async_copy(own_tile(s, k), vs.at[b, tile(k)], ld.at[k]).start())

        @pl.when(q != c)
        def _():
            each_tile(j, lambda k: pltpu.make_async_copy(vall.at[j, tile(k)], vs.at[b, tile(k)], ld.at[k]).start())

        each_tile(j, lambda k: pltpu.make_async_copy(vall.at[j, tile(k)], vs.at[b, tile(k)], ld.at[k]).wait())

    def project(j, p):
        ws[p] = jnp.zeros((NB, NB), jnp.float32)

        def add(k):
            ws[p] = ws[p] + mtm(vs[j % 2, tile(k), :], x[p, tile(k), :])

        each_tile(j, add)

    def update(j, p):
        def sub(k):
            x[p, tile(k), :] = x[p, tile(k), :] - mm(vs[j % 2, tile(k), :], ys[p])

        each_tile(j, sub)

    zl.wait()
    zc.wait()

    def lower(j):
        acquire(j)
        for p in range(2):
            project(j, p)
            ys[p] = mm(tb[j], ws[p])
            update(j, p)

    @pl.when(r == 1)
    def _():
        t_get(3)
        loop_down(4 * slots - 1, slots, lower)

    @pl.when(c < 2)
    def _():
        gc.wait()

        def add(s):
            gown[s] = gown[s] + grecv[s]

        loop_down(slots - 1, slots, add)
        factors()

        @pl.when(odd == 1)
        def _():
            loop_down(slots - 4, slots - 3, send_far)

    @pl.when(r == 1)
    def _():
        t_get(2)
        loop_down(3 * slots - 1, slots, lower)

    @pl.when(c == 0)
    def _():
        loop_down(slots - 1, slots, send_far)

    def w_copy(j, p):
        return remote(ws.at[p], wr.at[p, j % 2], w_s.at[p, j % 2], w_r.at[p, j % 2], (other, c))

    def finish(j, p):
        w_copy(j, p).wait()
        ys[p] = mm(tb[j], ws[p] + wr[p, j % 2])
        update(j, p)

    def both(j):
        acquire(j)
        project(j, 0)
        w_copy(j, 0).start()

        @pl.when(j < 2 * slots - 1)
        def _():
            finish(j + 1, 1)

        project(j, 1)
        w_copy(j, 1).start()
        finish(j, 0)

    t_get(1)
    t_get(0)
    loop_down(2 * slots - 1, 2 * slots, both)
    outs = [pltpu.make_async_copy(x.at[p], out_ref.at[:, pl.ds(p * NB, NB)], loc.at[p]) for p in range(2)]
    outs[0].start()
    finish(0, 1)
    outs[1].start()

    def sent(s):
        j = c * slots + s
        each_tile(j, lambda k: own_copy(s, k, far_s, far_r, far).wait_send())
        each_tile(j, lambda k: own_copy(s, k, sib_s, sib_r, sib).wait_send())
        each_tile(far * slots + s, lambda k: got_copy(far * slots + s, s, k, dia_s, dia_r, sib).wait_send())

    loop_down(slots - 1, slots, sent)

    @pl.when((r == 1) | (c < 2))
    def _():
        t_copy(c, 0, sib).wait_send()
        t_copy(c, 1, far).wait_send()

    @pl.when((r == 1) | (far < 2))
    def _():
        t_copy(far, 2, sib).wait_send()

    for o in outs:
        o.wait()


def solution(mesh):
    def local_program(v, t, z):
        rows, width = v.shape
        slots = width // NB
        f32 = jnp.float32
        any_spec = pl.BlockSpec(memory_space=pl.ANY)
        dma = pltpu.SemaphoreType.DMA
        out, _ = pl.pallas_call(
            kernel,
            out_shape=[jax.ShapeDtypeStruct((rows, 2 * NB), f32), jax.ShapeDtypeStruct((4 * slots, rows, NB), f32)],
            in_specs=[any_spec] * 3,
            out_specs=[any_spec] * 2,
            scratch_shapes=[
                pltpu.VMEM((2, rows, NB), f32),
                pltpu.VMEM((2, rows, NB), f32),
                pltpu.VMEM((4 * slots, NB, NB), f32),
                pltpu.VMEM((slots, NB, NB), f32),
                pltpu.VMEM((slots, NB, NB), f32),
                pltpu.VMEM(t.shape, f32),
                pltpu.VMEM((2, NB, NB), f32),
                pltpu.VMEM((2, 2, NB, NB), f32),
                pltpu.VMEM((2, NB, NB), f32),
                *[dma((slots, rows // TR))] * 6,
                dma((3,)), dma((3,)), dma((2, 2)), dma((2, 2)),
                dma, dma, dma, dma, dma((2,)), dma((rows // TR,)),
            ],
            compiler_params=pltpu.CompilerParams(collective_id=0, has_side_effects=True, vmem_limit_bytes=60 * 1024 * 1024),
        )(v, t, z)
        return out

    return jax.shard_map(local_program, mesh=mesh, in_specs=(P("row", "col"), P("col", None, None), P(None, ("col", "row"))), out_specs=P("row", "col"), check_vma=False)
```

```python
import jax
import jax.numpy as jnp
from jax import lax
from jax.experimental import pallas as pl
from jax.experimental.pallas import tpu as pltpu
from jax.sharding import PartitionSpec as P

FULL = lax.Precision.HIGHEST
MESH = pl.DeviceIdType.MESH
NB = 256
TR = 512


def mm(a, b):
    return lax.dot_general(a, b, (((1,), (0,)), ((), ())), precision=FULL, preferred_element_type=jnp.float32)


def mtm(a, b):
    return lax.dot_general(a, b, (((0,), (0,)), ((), ())), precision=FULL, preferred_element_type=jnp.float32)


def kernel(
    v_ref, t_ref, z_ref, out_ref, vall,
    x, vs, tb, gown, grecv, ts, ws, wr, ys, w2, y2,
    far_s, far_r, sib_s, sib_r, dia_s, dia_r, up_s, up_r, down_s, t_s, t_r, w_s, w_r, z_s, z_r, g_s, g_r, loc, ld,
):
    r = lax.axis_index("row")
    c = lax.axis_index("col")
    rows = v_ref.shape[0]
    slots = v_ref.shape[1] // NB
    tiles = rows // TR
    per_row = rows // NB
    sib = c + 1 - 2 * (c % 2)
    far = (c + 2) % 4
    other = 1 - r

    barrier = pltpu.get_barrier_semaphore()
    for dst in ((r, sib), (r, far), (other, c), (other, far)):
        pl.semaphore_signal(barrier, inc=1, device_id=dst, device_id_type=MESH)
    pl.semaphore_wait(barrier, 4)

    def first_tile(j):
        return lax.min(lax.max(j - per_row * r, 0) * NB // TR, tiles)

    def tile(k):
        return pl.ds(pl.multiple_of(k * TR, TR), TR)

    def each_tile(j, fn):
        def body(k, carry):
            fn(k)
            return carry

        lax.fori_loop(first_tile(j), tiles, body, 0)

    def own_tile(s, k):
        return v_ref.at[tile(k), pl.ds(pl.multiple_of(s * NB, NB), NB)]

    def remote(src, dst, ssem, rsem, to):
        return pltpu.make_async_remote_copy(src_ref=src, dst_ref=dst, send_sem=ssem, recv_sem=rsem, device_id=to, device_id_type=MESH)

    def own_copy(s, k, ssem, rsem, to, to_row=r):
        return remote(own_tile(s, k), vall.at[c * slots + s, tile(k)], ssem.at[s, k], rsem.at[s, k], (to_row, to))

    def got_copy(j, s, k, ssem, rsem, to):
        return remote(vall.at[j, tile(k)], vall.at[j, tile(k)], ssem.at[s, k], rsem.at[s, k], (r, to))

    def by_row0(j, k):
        upper = (j >= per_row) & (k % 3 == 2)
        lower_part = (j < per_row) & ((k == 5) | ((k == 2) & (j % 4 == 3)))
        return (j < 0) & upper & lower_part

    def direct_tile(s, fn):
        j = c * slots + s

        def body(k):
            @pl.when(jnp.logical_not((r == 1) & by_row0(j, k)))
            def _():
                fn(k)

        each_tile(j, body)

    def relay_tile(s, fn):
        j = c * slots + s

        def body(k, carry):
            @pl.when(by_row0(j, k))
            def _():
                fn(k)

            return carry

        lax.fori_loop(lax.max(j - per_row, 0) * NB // TR, tiles, body, 0)

    def up_copy(s, k):
        return own_copy(s, k, up_s, up_r, c, other)

    def down_copy(s, k):
        part = vall.at[c * slots + s, tile(k)]
        return remote(part, part, down_s.at[s, k], far_r.at[s, k], (other, far))

    def send_far(s):
        direct_tile(s, lambda k: own_copy(s, k, far_s, far_r, far).start())

    def send_up(s):
        relay_tile(s, lambda k: up_copy(s, k).start())

    def relay(s):
        def fn(k):
            up_copy(s, k).wait_recv()
            down_copy(s, k).start()

        relay_tile(s, fn)

    def loop_down(hi, n, fn):
        def body(i, carry):
            fn(hi - i)
            return carry

        lax.fori_loop(0, n, body, 0)

    zc = remote(z_ref.at[pl.ds(pl.multiple_of(other * rows, rows), rows)], x.at[:, pl.ds(pl.multiple_of(r * NB, NB), NB)], z_s, z_r, (other, c))

    @pl.when(r == 0)
    def _():
        zc.start()

    zl = pltpu.make_async_copy(z_ref.at[pl.ds(pl.multiple_of(r * rows, rows), rows)], x.at[:, pl.ds(pl.multiple_of(r * NB, NB), NB)], loc.at[0])
    zl.start()
    tl = pltpu.make_async_copy(t_ref, ts, loc.at[1])
    tl.start()

    odd = c % 2

    @pl.when((r == 1) & (c >= 2))
    def _():
        loop_down(slots - 1, slots, send_up)
        zc.start()

    @pl.when(odd == 1)
    def _():
        loop_down(slots - 1, slots, send_far)

    loop_down(slots - 1, slots, lambda s: each_tile(c * slots + s, lambda k: own_copy(s, k, sib_s, sib_r, sib).start()))

    def gram_load(s, k):
        return pltpu.make_async_copy(own_tile(s, k), vs.at[s % 2, tile(k)], ld.at[s % 2, k])

    def gram(s):
        j = c * slots + s

        @pl.when(s > 0)
        def _():
            each_tile(j - 1, lambda k: gram_load(s - 1, k).start())

        gown[s] = jnp.zeros((NB, NB), jnp.float32)

        def add(k):
            gram_load(s, k).wait()
            v_t = vs[s % 2, tile(k), :]
            gown[s] = gown[s] + mtm(v_t, v_t)

        each_tile(j, add)

    each_tile(c * slots + slots - 1, lambda k: gram_load(slots - 1, k).start())
    loop_down(slots - 1, slots, gram)
    tl.wait()

    def merge():
        quarter = range(0, NB, 128)
        for s in range(slots):
            tb[c * slots + s] = jnp.zeros((NB, NB), jnp.float32)
        t64 = [[ts[4 * s + i] for i in range(4)] for s in range(slots)]
        u64 = [[mm(t64[s][o // 64], gown[s, o : o + 64, o + 64 : o + 128]) for o in quarter] for s in range(slots)]
        n64 = [[-mm(u64[s][i], t64[s][2 * i + 1]) for i in range(2)] for s in range(slots)]
        for s in range(slots):
            j = c * slots + s
            for i, o in enumerate(quarter):
                tb[j, o : o + 64, o : o + 64] = t64[s][2 * i]
                tb[j, o + 64 : o + 128, o + 64 : o + 128] = t64[s][2 * i + 1]
                tb[j, o : o + 64, o + 64 : o + 128] = n64[s][i]
        u128 = [mm(tb[c * slots + s, 0:128, 0:128], gown[s, 0:128, 128:256]) for s in range(slots)]
        for s in range(slots):
            j = c * slots + s
            tb[j, 0:128, 128:256] = -mm(u128[s], tb[j, 128:256, 128:256])

    def t_sib(q):
        part = tb.at[pl.ds(q * slots, slots)]
        return remote(part, part, t_s.at[0], t_r.at[0], (r, sib))

    def t_chip(x_of, i, to):
        part = tb.at[pl.ds(x_of * 2 * slots, 2 * slots)]
        return remote(part, part, t_s.at[i], t_r.at[i], (r, to))

    chip = c // 2

    def factors():
        merge()
        t_sib(c).start()
        t_sib(sib).wait_recv()

        @pl.when(odd == 0)
        def _():
            t_chip(chip, 1, far).start()

    gc = remote(gown, grecv, g_s, g_r, (other, c))

    @pl.when(c < 2)
    def _():
        gc.start()

    @pl.when((r == 1) & (c < 2))
    def _():
        loop_down(slots - 1, slots, send_up)
        zc.start()

    @pl.when((c >= 2) & (r == 1))
    def _():
        factors()

    @pl.when(c == 2)
    def _():
        loop_down(slots - 1, slots, send_far)

    def t_far():
        @pl.when(odd == 0)
        def _():
            t_chip(1 - chip, 1, far).wait_recv()
            t_chip(1 - chip, 2, sib).start()

        @pl.when(odd == 1)
        def _():
            t_chip(1 - chip, 2, sib).wait_recv()

    def load(j, k):
        return pltpu.make_async_copy(vall.at[j, tile(k)], vs.at[j % 2, tile(k)], ld.at[j % 2, k])

    def arrive(j):
        q, s = j // slots, j % slots

        @pl.when(q == c)
        def _():
            each_tile(j, lambda k: pltpu.make_async_copy(own_tile(s, k), vs.at[j % 2, tile(k)], ld.at[j % 2, k]).start())

        @pl.when(q == sib)
        def _():
            def fn(k):
                got_copy(j, s, k, sib_s, sib_r, sib).wait_recv()
                load(j, k).start()

            each_tile(j, fn)

        @pl.when(q == far)
        def _():
            def fn(k):
                got_copy(j, s, k, far_s, far_r, far).wait_recv()
                got_copy(j, s, k, dia_s, dia_r, sib).start()
                load(j, k).start()

            each_tile(j, fn)

        @pl.when((q + 2) % 4 == sib)
        def _():
            def fn(k):
                got_copy(j, s, k, dia_s, dia_r, sib).wait_recv()
                load(j, k).start()

            each_tile(j, fn)

    def ahead(j):
        return (j // slots // 2 == c // 2) & (j % slots != slots - 1)

    def ready(j):
        @pl.when(jnp.logical_not(ahead(j)))
        def _():
            arrive(j)

        each_tile(j, lambda k: load(j, k).wait())

    def next_load(j):
        @pl.when((j % slots != 0) & ahead(j - 1))
        def _():
            arrive(j - 1)

    def tile_pairs(j, fn):
        lo = first_tile(j)

        @pl.when(lo % 2 == 1)
        def _():
            fn(tile(lo))

        def body(i, carry):
            fn(pl.ds(pl.multiple_of(i * 2 * TR, 2 * TR), 2 * TR))
            return carry

        lax.fori_loop((lo + 1) // 2, tiles // 2, body, 0)

    def project(j, p):
        ws[p] = jnp.zeros((NB, NB), jnp.float32)

        def add(rng):
            ws[p] = ws[p] + mtm(vs[j % 2, rng, :], x[rng, p * NB : (p + 1) * NB])

        tile_pairs(j, add)

    def update(j, p):
        def sub(rng):
            x[rng, p * NB : (p + 1) * NB] = x[rng, p * NB : (p + 1) * NB] - mm(vs[j % 2, rng, :], ys[p])

        tile_pairs(j, sub)

    zl.wait()

    @pl.when((r == 0) & (c >= 2))
    def _():
        loop_down(slots - 1, slots, relay)

    @pl.when(r == 1)
    def _():
        zc.wait()

    def lower(j):
        ready(j)
        next_load(j)
        w2[...] = jnp.zeros_like(w2)

        def add(rng):
            w2[...] = w2[...] + mtm(vs[j % 2, rng, :], x[rng, :])

        tile_pairs(j, add)
        y2[...] = mm(tb[j], w2[...])

        def sub(rng):
            x[rng, :] = x[rng, :] - mm(vs[j % 2, rng, :], y2[...])

        tile_pairs(j, sub)

        @pl.when((c == 0) & (j < 3 * slots))
        def _():
            send_far(j - 2 * slots)

    @pl.when(r == 1)
    def _():
        @pl.when(c < 2)
        def _():
            t_far()

        loop_down(4 * slots - 1, slots, lower)

    @pl.when(c < 2)
    def _():
        gc.wait()

        def add(s):
            gown[s] = gown[s] + grecv[s]

        loop_down(slots - 1, slots, add)
        factors()

    @pl.when((r == 0) & (c == 0))
    def _():
        loop_down(slots - 1, slots, send_far)

    @pl.when((r == 0) & (c < 2))
    def _():
        loop_down(slots - 1, slots, relay)

    @pl.when(r == 1)
    def _():
        loop_down(3 * slots - 1, slots, lower)

    def w_copy(j, p):
        return remote(ws.at[p], wr.at[p, j % 2], w_s.at[p, j % 2], w_r.at[p, j % 2], (other, c))

    def finish(j, p):
        w_copy(j, p).wait()
        ys[p] = mm(tb[j], ws[p] + wr[p, j % 2])
        update(j, p)

    def both(j):
        ready(j)
        project(j, 0)
        w_copy(j, 0).start()

        @pl.when(j < 2 * slots - 1)
        def _():
            finish(j + 1, 1)

        next_load(j)
        project(j, 1)
        w_copy(j, 1).start()
        finish(j, 0)

    @pl.when(r == 0)
    def _():
        zc.wait()

    @pl.when(c >= 2)
    def _():
        t_far()

    loop_down(2 * slots - 1, 2 * slots, both)
    outs = [pltpu.make_async_copy(x.at[:, pl.ds(p * NB, NB)], out_ref.at[:, pl.ds(p * NB, NB)], loc.at[p]) for p in range(2)]
    outs[0].start()
    finish(0, 1)
    outs[1].start()

    def sent(s):
        j = c * slots + s
        direct_tile(s, lambda k: own_copy(s, k, far_s, far_r, far).wait_send())

        @pl.when(r == 1)
        def _():
            relay_tile(s, lambda k: up_copy(s, k).wait_send())

        @pl.when(r == 0)
        def _():
            relay_tile(s, lambda k: down_copy(s, k).wait_send())

        each_tile(j, lambda k: own_copy(s, k, sib_s, sib_r, sib).wait_send())
        each_tile(far * slots + s, lambda k: got_copy(far * slots + s, s, k, dia_s, dia_r, sib).wait_send())

    loop_down(slots - 1, slots, sent)

    @pl.when((r == 1) | (c < 2))
    def _():
        t_sib(c).wait_send()

        @pl.when(odd == 0)
        def _():
            t_chip(chip, 1, far).wait_send()

    @pl.when(((r == 1) | (c >= 2)) & (odd == 0))
    def _():
        t_chip(1 - chip, 2, sib).wait_send()

    for o in outs:
        o.wait()


def solution(mesh):
    def local_program(v, t, z):
        rows, width = v.shape
        slots = width // NB
        f32 = jnp.float32
        any_spec = pl.BlockSpec(memory_space=pl.ANY)
        dma = pltpu.SemaphoreType.DMA
        out, _ = pl.pallas_call(
            kernel,
            out_shape=[jax.ShapeDtypeStruct((rows, 2 * NB), f32), jax.ShapeDtypeStruct((4 * slots, rows, NB), f32)],
            in_specs=[any_spec] * 3,
            out_specs=[any_spec] * 2,
            scratch_shapes=[
                pltpu.VMEM((rows, 2 * NB), f32),
                pltpu.VMEM((2, rows, NB), f32),
                pltpu.VMEM((4 * slots, NB, NB), f32),
                pltpu.VMEM((slots, NB, NB), f32),
                pltpu.VMEM((slots, NB, NB), f32),
                pltpu.VMEM(t.shape, f32),
                pltpu.VMEM((2, NB, NB), f32),
                pltpu.VMEM((2, 2, NB, NB), f32),
                pltpu.VMEM((2, NB, NB), f32),
                pltpu.VMEM((NB, 2 * NB), f32),
                pltpu.VMEM((NB, 2 * NB), f32),
                *[dma((slots, rows // TR))] * 9,
                dma((3,)), dma((3,)), dma((2, 2)), dma((2, 2)),
                dma, dma, dma, dma, dma((2,)), dma((2, rows // TR)),
            ],
            compiler_params=pltpu.CompilerParams(collective_id=0, has_side_effects=True, vmem_limit_bytes=60 * 1024 * 1024),
        )(v, t, z)
        return out

    return jax.shard_map(local_program, mesh=mesh, in_specs=(P("row", "col"), P("col", None, None), P(None, ("col", "row"))), out_specs=P("row", "col"), check_vma=False)
```

```python
import jax
import jax.numpy as jnp
from jax import lax
from jax.experimental import pallas as pl
from jax.experimental.pallas import tpu as pltpu
from jax.sharding import PartitionSpec as P

FULL = lax.Precision.HIGHEST
MESH = pl.DeviceIdType.MESH
NB = 256
TR = 512


def mm(a, b):
    return lax.dot_general(a, b, (((1,), (0,)), ((), ())), precision=FULL, preferred_element_type=jnp.float32)


def mtm(a, b):
    return lax.dot_general(a, b, (((0,), (0,)), ((), ())), precision=FULL, preferred_element_type=jnp.float32)


def kernel(
    v_ref, t_ref, z_ref, out_ref, vall,
    x, vs, tb, gown, grecv, ts, ws, wr, ys, w2, y2,
    far_s, far_r, sib_s, sib_r, dia_s, dia_r, up_s, up_r, down_s, t_s, t_r, w_s, w_r, z_s, z_r, g_s, g_r, loc, ld,
):
    r = lax.axis_index("row")
    c = lax.axis_index("col")
    rows = v_ref.shape[0]
    slots = v_ref.shape[1] // NB
    tiles = rows // TR
    per_row = rows // NB
    sib = c + 1 - 2 * (c % 2)
    far = (c + 2) % 4
    other = 1 - r

    barrier = pltpu.get_barrier_semaphore()
    for dst in ((r, sib), (r, far), (other, c), (other, far)):
        pl.semaphore_signal(barrier, inc=1, device_id=dst, device_id_type=MESH)
    pl.semaphore_wait(barrier, 4)

    def first_tile(j):
        return lax.min(lax.max(j - per_row * r, 0) * NB // TR, tiles)

    def tile(k):
        return pl.ds(pl.multiple_of(k * TR, TR), TR)

    def each_tile(j, fn):
        def body(k, carry):
            fn(k)
            return carry

        lax.fori_loop(first_tile(j), tiles, body, 0)

    def own_tile(s, k):
        return v_ref.at[tile(k), pl.ds(pl.multiple_of(s * NB, NB), NB)]

    def remote(src, dst, ssem, rsem, to):
        return pltpu.make_async_remote_copy(src_ref=src, dst_ref=dst, send_sem=ssem, recv_sem=rsem, device_id=to, device_id_type=MESH)

    def own_copy(s, k, ssem, rsem, to, to_row=r):
        return remote(own_tile(s, k), vall.at[c * slots + s, tile(k)], ssem.at[s, k], rsem.at[s, k], (to_row, to))

    def got_copy(j, s, k, ssem, rsem, to):
        return remote(vall.at[j, tile(k)], vall.at[j, tile(k)], ssem.at[s, k], rsem.at[s, k], (r, to))

    def by_row0(j, k):
        upper = (j >= per_row) & (j < 3 * slots) & (k % 3 == 2)
        lower_part = (j < per_row) & ((k == 5) | ((k == 2) & (j % 4 == 3)))
        return upper | ((j >= slots) & (j < 2 * slots) & (k == 5))

    def direct_tile(s, fn):
        j = c * slots + s

        def body(k):
            @pl.when(jnp.logical_not((r == 1) & by_row0(j, k)))
            def _():
                fn(k)

        each_tile(j, body)

    def relay_tile(s, fn):
        j = c * slots + s

        def body(k, carry):
            @pl.when(by_row0(j, k))
            def _():
                fn(k)

            return carry

        lax.fori_loop(lax.max(j - per_row, 0) * NB // TR, tiles, body, 0)

    def up_copy(s, k):
        return own_copy(s, k, up_s, up_r, c, other)

    def down_copy(s, k):
        part = vall.at[c * slots + s, tile(k)]
        return remote(part, part, down_s.at[s, k], far_r.at[s, k], (other, far))

    def send_far(s):
        direct_tile(s, lambda k: own_copy(s, k, far_s, far_r, far).start())

    def send_up(s):
        relay_tile(s, lambda k: up_copy(s, k).start())

    def relay(s):
        def fn(k):
            up_copy(s, k).wait_recv()
            down_copy(s, k).start()

        relay_tile(s, fn)

    def loop_down(hi, n, fn):
        def body(i, carry):
            fn(hi - i)
            return carry

        lax.fori_loop(0, n, body, 0)

    zc = remote(z_ref.at[pl.ds(pl.multiple_of(other * rows, rows), rows)], x.at[:, pl.ds(pl.multiple_of(r * NB, NB), NB)], z_s, z_r, (other, c))

    @pl.when(r == 0)
    def _():
        zc.start()

    zl = pltpu.make_async_copy(z_ref.at[pl.ds(pl.multiple_of(r * rows, rows), rows)], x.at[:, pl.ds(pl.multiple_of(r * NB, NB), NB)], loc.at[0])
    zl.start()
    tl = pltpu.make_async_copy(t_ref, ts, loc.at[1])
    tl.start()

    odd = c % 2

    @pl.when((r == 1) & (c >= 1))
    def _():
        loop_down(slots - 1, slots, send_up)

    @pl.when((r == 1) & (c >= 2))
    def _():
        zc.start()

    @pl.when(odd == 1)
    def _():
        loop_down(slots - 1, slots, send_far)

    loop_down(slots - 1, slots, lambda s: each_tile(c * slots + s, lambda k: own_copy(s, k, sib_s, sib_r, sib).start()))

    def gram_load(s, k):
        return pltpu.make_async_copy(own_tile(s, k), vs.at[s % 2, tile(k)], ld.at[s % 2, k])

    def gram(s):
        j = c * slots + s

        @pl.when(s > 0)
        def _():
            each_tile(j - 1, lambda k: gram_load(s - 1, k).start())

        gown[s] = jnp.zeros((NB, NB), jnp.float32)

        def add(k):
            gram_load(s, k).wait()
            v_t = vs[s % 2, tile(k), :]
            gown[s] = gown[s] + mtm(v_t, v_t)

        each_tile(j, add)

    each_tile(c * slots + slots - 1, lambda k: gram_load(slots - 1, k).start())
    loop_down(slots - 1, slots, gram)
    tl.wait()

    def merge():
        quarter = range(0, NB, 128)
        for s in range(slots):
            tb[c * slots + s] = jnp.zeros((NB, NB), jnp.float32)
        t64 = [[ts[4 * s + i] for i in range(4)] for s in range(slots)]
        u64 = [[mm(t64[s][o // 64], gown[s, o : o + 64, o + 64 : o + 128]) for o in quarter] for s in range(slots)]
        n64 = [[-mm(u64[s][i], t64[s][2 * i + 1]) for i in range(2)] for s in range(slots)]
        for s in range(slots):
            j = c * slots + s
            for i, o in enumerate(quarter):
                tb[j, o : o + 64, o : o + 64] = t64[s][2 * i]
                tb[j, o + 64 : o + 128, o + 64 : o + 128] = t64[s][2 * i + 1]
                tb[j, o : o + 64, o + 64 : o + 128] = n64[s][i]
        u128 = [mm(tb[c * slots + s, 0:128, 0:128], gown[s, 0:128, 128:256]) for s in range(slots)]
        for s in range(slots):
            j = c * slots + s
            tb[j, 0:128, 128:256] = -mm(u128[s], tb[j, 128:256, 128:256])

    def t_sib(q):
        part = tb.at[pl.ds(q * slots, slots)]
        return remote(part, part, t_s.at[0], t_r.at[0], (r, sib))

    def t_chip(x_of, i, to):
        part = tb.at[pl.ds(x_of * 2 * slots, 2 * slots)]
        return remote(part, part, t_s.at[i], t_r.at[i], (r, to))

    chip = c // 2

    def factors():
        merge()
        t_sib(c).start()
        t_sib(sib).wait_recv()

        @pl.when(odd == 0)
        def _():
            t_chip(chip, 1, far).start()

    gc = remote(gown, grecv, g_s, g_r, (other, c))

    @pl.when(c < 2)
    def _():
        gc.start()

    @pl.when((r == 1) & (c == 0))
    def _():
        loop_down(slots - 1, slots, send_up)

    @pl.when((r == 1) & (c < 2))
    def _():
        zc.start()

    @pl.when((c >= 2) & (r == 1))
    def _():
        factors()

    @pl.when(c == 2)
    def _():
        loop_down(slots - 1, slots, send_far)

    def t_far():
        @pl.when(odd == 0)
        def _():
            t_chip(1 - chip, 1, far).wait_recv()
            t_chip(1 - chip, 2, sib).start()

        @pl.when(odd == 1)
        def _():
            t_chip(1 - chip, 2, sib).wait_recv()

    def load(j, k):
        return pltpu.make_async_copy(vall.at[j, tile(k)], vs.at[j % 2, tile(k)], ld.at[j % 2, k])

    def arrive(j):
        q, s = j // slots, j % slots

        @pl.when(q == c)
        def _():
            each_tile(j, lambda k: pltpu.make_async_copy(own_tile(s, k), vs.at[j % 2, tile(k)], ld.at[j % 2, k]).start())

        @pl.when(q == sib)
        def _():
            def fn(k):
                got_copy(j, s, k, sib_s, sib_r, sib).wait_recv()
                load(j, k).start()

            each_tile(j, fn)

        @pl.when(q == far)
        def _():
            def fn(k):
                got_copy(j, s, k, far_s, far_r, far).wait_recv()
                got_copy(j, s, k, dia_s, dia_r, sib).start()
                load(j, k).start()

            each_tile(j, fn)

        @pl.when((q + 2) % 4 == sib)
        def _():
            def fn(k):
                got_copy(j, s, k, dia_s, dia_r, sib).wait_recv()
                load(j, k).start()

            each_tile(j, fn)

    def ahead(j):
        return (j // slots // 2 == c // 2) & (j % slots != slots - 1)

    def ready(j):
        @pl.when(jnp.logical_not(ahead(j)))
        def _():
            arrive(j)

        each_tile(j, lambda k: load(j, k).wait())

    def next_load(j):
        @pl.when((j % slots != 0) & ahead(j - 1))
        def _():
            arrive(j - 1)

    def tile_pairs(j, fn):
        lo = first_tile(j)

        @pl.when(lo % 2 == 1)
        def _():
            fn(tile(lo))

        def body(i, carry):
            fn(pl.ds(pl.multiple_of(i * 2 * TR, 2 * TR), 2 * TR))
            return carry

        lax.fori_loop((lo + 1) // 2, tiles // 2, body, 0)

    def project(j, p):
        ws[p] = jnp.zeros((NB, NB), jnp.float32)

        def add(rng):
            ws[p] = ws[p] + mtm(vs[j % 2, rng, :], x[rng, p * NB : (p + 1) * NB])

        tile_pairs(j, add)

    def update(j, p):
        def sub(rng):
            x[rng, p * NB : (p + 1) * NB] = x[rng, p * NB : (p + 1) * NB] - mm(vs[j % 2, rng, :], ys[p])

        tile_pairs(j, sub)

    zl.wait()

    @pl.when((r == 0) & (c >= 1))
    def _():
        loop_down(slots - 1, slots, relay)

    @pl.when(r == 1)
    def _():
        zc.wait()

    def lower(j):
        ready(j)
        next_load(j)
        w2[...] = jnp.zeros_like(w2)

        def add(rng):
            w2[...] = w2[...] + mtm(vs[j % 2, rng, :], x[rng, :])

        tile_pairs(j, add)
        y2[...] = mm(tb[j], w2[...])

        def sub(rng):
            x[rng, :] = x[rng, :] - mm(vs[j % 2, rng, :], y2[...])

        tile_pairs(j, sub)

        @pl.when((c == 0) & (j < 3 * slots))
        def _():
            send_far(j - 2 * slots)

    @pl.when(r == 1)
    def _():
        @pl.when(c < 2)
        def _():
            t_far()

        loop_down(4 * slots - 1, slots, lower)

    @pl.when(c < 2)
    def _():
        gc.wait()

        def add(s):
            gown[s] = gown[s] + grecv[s]

        loop_down(slots - 1, slots, add)
        factors()

    @pl.when((r == 0) & (c == 0))
    def _():
        loop_down(slots - 1, slots, relay)
        loop_down(slots - 1, slots, send_far)

    @pl.when(r == 1)
    def _():
        loop_down(3 * slots - 1, slots, lower)

    def w_copy(j, p):
        return remote(ws.at[p], wr.at[p, j % 2], w_s.at[p, j % 2], w_r.at[p, j % 2], (other, c))

    def finish(j, p):
        w_copy(j, p).wait()
        ys[p] = mm(tb[j], ws[p] + wr[p, j % 2])
        update(j, p)

    def both(j):
        ready(j)
        project(j, 0)
        w_copy(j, 0).start()

        @pl.when(j < 2 * slots - 1)
        def _():
            finish(j + 1, 1)

        next_load(j)
        project(j, 1)
        w_copy(j, 1).start()
        finish(j, 0)

    @pl.when(r == 0)
    def _():
        zc.wait()

    @pl.when(c >= 2)
    def _():
        t_far()

    loop_down(2 * slots - 1, 2 * slots, both)
    outs = [pltpu.make_async_copy(x.at[:, pl.ds(p * NB, NB)], out_ref.at[:, pl.ds(p * NB, NB)], loc.at[p]) for p in range(2)]
    outs[0].start()
    finish(0, 1)
    outs[1].start()

    def sent(s):
        j = c * slots + s
        direct_tile(s, lambda k: own_copy(s, k, far_s, far_r, far).wait_send())

        @pl.when(r == 1)
        def _():
            relay_tile(s, lambda k: up_copy(s, k).wait_send())

        @pl.when(r == 0)
        def _():
            relay_tile(s, lambda k: down_copy(s, k).wait_send())

        each_tile(j, lambda k: own_copy(s, k, sib_s, sib_r, sib).wait_send())
        each_tile(far * slots + s, lambda k: got_copy(far * slots + s, s, k, dia_s, dia_r, sib).wait_send())

    loop_down(slots - 1, slots, sent)

    @pl.when((r == 1) | (c < 2))
    def _():
        t_sib(c).wait_send()

        @pl.when(odd == 0)
        def _():
            t_chip(chip, 1, far).wait_send()

    @pl.when(((r == 1) | (c >= 2)) & (odd == 0))
    def _():
        t_chip(1 - chip, 2, sib).wait_send()

    for o in outs:
        o.wait()


def solution(mesh):
    def local_program(v, t, z):
        rows, width = v.shape
        slots = width // NB
        f32 = jnp.float32
        any_spec = pl.BlockSpec(memory_space=pl.ANY)
        dma = pltpu.SemaphoreType.DMA
        out, _ = pl.pallas_call(
            kernel,
            out_shape=[jax.ShapeDtypeStruct((rows, 2 * NB), f32), jax.ShapeDtypeStruct((4 * slots, rows, NB), f32)],
            in_specs=[any_spec] * 3,
            out_specs=[any_spec] * 2,
            scratch_shapes=[
                pltpu.VMEM((rows, 2 * NB), f32),
                pltpu.VMEM((2, rows, NB), f32),
                pltpu.VMEM((4 * slots, NB, NB), f32),
                pltpu.VMEM((slots, NB, NB), f32),
                pltpu.VMEM((slots, NB, NB), f32),
                pltpu.VMEM(t.shape, f32),
                pltpu.VMEM((2, NB, NB), f32),
                pltpu.VMEM((2, 2, NB, NB), f32),
                pltpu.VMEM((2, NB, NB), f32),
                pltpu.VMEM((NB, 2 * NB), f32),
                pltpu.VMEM((NB, 2 * NB), f32),
                *[dma((slots, rows // TR))] * 9,
                dma((3,)), dma((3,)), dma((2, 2)), dma((2, 2)),
                dma, dma, dma, dma, dma((2,)), dma((2, rows // TR)),
            ],
            compiler_params=pltpu.CompilerParams(collective_id=0, has_side_effects=True, vmem_limit_bytes=60 * 1024 * 1024),
        )(v, t, z)
        return out

    return jax.shard_map(local_program, mesh=mesh, in_specs=(P("row", "col"), P("col", None, None), P(None, ("col", "row"))), out_specs=P("row", "col"), check_vma=False)
```
